16 devices in a mesh: data: 2 (over z), seq: 8 (over y, x, core).
Axes of the slice: x: 2, y: 2, z: 2, core: 2. Of those that a mesh axis runs over, the one named last changes fastest.
Arguments:
- x_in: bfloat16 [16, 1024, 2048], P(None, ('data', 'seq')), parts along dimension 1
- positions: int32 [1024], P(('data', 'seq')), parts along dimension 0
- w_query: bfloat16 [3, 2048, 32, 64], replicated
- w_key: bfloat16 [3, 2048, 8, 64], replicated
- w_value: bfloat16 [3, 2048, 8, 64], replicated
- w_out: bfloat16 [3, 32, 64, 2048], replicated
- w_up: bfloat16 [3, 2048, 8192], replicated
- w_down: bfloat16 [3, 8192, 2048], replicated
- g_attn: float32 [3, 2048], replicated
- g_mlp: float32 [3, 2048], replicated
Outputs:
- output: bfloat16 [16, 1024, 2048], P(None, ('data', 'seq')), parts along dimension 1
There are 2 independent parts. The reference program is written for one: setup_inputs(seed, part) draws one part's arguments, and reference() takes and returns one part's arrays. A program takes and returns all parts, laid end to end along the dimension named above; an argument that names none is the same for every part.
All inputs are finite; a program needn't handle non-finite values.
Results may differ from the reference program's by a relative error of at most 0.0166204.
Values are sent between devices in bfloat16 or wider.
A program may use at most 1.25 GiB of HBM per device.

```python
import jax
import jax.numpy as jnp
from jax import lax

BATCH_SIZE = 16
SEQ_LEN = 512
D_MODEL = 2048
N_HEADS = 32
N_KV_HEADS = 8
HEAD_DIM = 64
FF_DIM = 8192
N_LAYERS = 3
REF_BLOCK = 64

ROPE_BASE = 10000.0
NORM_EPS = 1e-6


def normal_weights(rng_key, w_shape, fan_in, w_gain):
    return (jax.random.normal(rng_key, w_shape, jnp.float32) * (w_gain * fan_in ** -0.5)).astype(jnp.bfloat16)


def setup_inputs(seed: int = 0, part: int = 0) -> dict:
    base_key = jax.random.key(seed)
    part_keys = jax.random.split(jax.random.fold_in(base_key, part), 6)
    weight_keys = jax.random.split(jax.random.fold_in(base_key, 100003), 8)
    step_frac = jnp.arange(SEQ_LEN, dtype=jnp.float32) / SEQ_LEN
    wave_freq = jax.random.uniform(part_keys[0], (BATCH_SIZE, 4), jnp.float32, minval=0.5, maxval=3.0)
    wave_phase = jax.random.uniform(part_keys[1], (BATCH_SIZE, 4), jnp.float32, minval=0.0, maxval=6.283185)
    wave_vals = jnp.cos(6.283185 * wave_freq[:, :, None] * step_frac[None, None, :] + wave_phase[:, :, None])
    wave_dirs = jax.random.normal(part_keys[2], (BATCH_SIZE, 4, D_MODEL), jnp.float32)
    smooth = jnp.einsum("bjs,bjd->bsd", wave_vals, wave_dirs) * 0.5
    noise_part = jax.random.normal(part_keys[3], (BATCH_SIZE, SEQ_LEN, D_MODEL), jnp.float32) * 0.7
    offset = jax.random.randint(part_keys[4], (), 0, SEQ_LEN)
    pos_gaps = jax.random.randint(part_keys[5], (SEQ_LEN,), 1, 5)
    return {
        "x_in": (smooth + noise_part).astype(jnp.bfloat16),
        "positions": (offset + jnp.cumsum(pos_gaps)).astype(jnp.int32),
        "w_query": normal_weights(weight_keys[0], (N_LAYERS, D_MODEL, N_HEADS, HEAD_DIM), D_MODEL, 1.25),
        "w_key": normal_weights(weight_keys[1], (N_LAYERS, D_MODEL, N_KV_HEADS, HEAD_DIM), D_MODEL, 1.25),
        "w_value": normal_weights(weight_keys[2], (N_LAYERS, D_MODEL, N_KV_HEADS, HEAD_DIM), D_MODEL, 1.0),
        "w_out": normal_weights(weight_keys[3], (N_LAYERS, N_HEADS, HEAD_DIM, D_MODEL), N_HEADS * HEAD_DIM, 1.0),
        "w_up": normal_weights(weight_keys[4], (N_LAYERS, D_MODEL, FF_DIM), D_MODEL, 1.0),
        "w_down": normal_weights(weight_keys[5], (N_LAYERS, FF_DIM, D_MODEL), FF_DIM, 1.0),
        "g_attn": jax.random.uniform(weight_keys[6], (N_LAYERS, D_MODEL), jnp.float32, minval=0.5, maxval=1.5),
        "g_mlp": jax.random.uniform(weight_keys[7], (N_LAYERS, D_MODEL), jnp.float32, minval=0.5, maxval=1.5),
    }


def rms_norm(x_act, gain_vec):
    x_f32 = x_act.astype(jnp.float32)
    mean_sq = jnp.mean(x_f32 * x_f32, axis=-1, keepdims=True)
    return (x_f32 * lax.rsqrt(mean_sq + NORM_EPS) * gain_vec).astype(jnp.bfloat16)


def rope_tables(positions):
    inv_freq = ROPE_BASE ** (-jnp.arange(HEAD_DIM // 2, dtype=jnp.float32) * (2.0 / HEAD_DIM))
    angles = positions.astype(jnp.float32)[:, None] * inv_freq[None, :]
    return jnp.cos(angles), jnp.sin(angles)


def apply_rope(proj_f32, cos_t, sin_t):
    half_dim = HEAD_DIM // 2
    x_first = proj_f32[..., :half_dim]
    x_second = proj_f32[..., half_dim:]
    cos_b = cos_t[:, None, :]
    sin_b = sin_t[:, None, :]
    return jnp.concatenate([x_first * cos_b - x_second * sin_b, x_second * cos_b + x_first * sin_b], axis=-1).astype(jnp.bfloat16)


def causal_attention(q_heads, k_heads, v_heads):
    groups = N_HEADS // N_KV_HEADS
    n_blocks = SEQ_LEN // REF_BLOCK
    att_scale = HEAD_DIM ** -0.5
    q_grouped = q_heads.reshape(BATCH_SIZE, SEQ_LEN, N_KV_HEADS, groups, HEAD_DIM)
    k_f32 = k_heads.astype(jnp.float32)
    v_f32 = v_heads.astype(jnp.float32)
    key_pos = jnp.arange(SEQ_LEN)

    def one_block(blk_idx):
        blk_start = blk_idx * REF_BLOCK
        q_blk = lax.dynamic_slice_in_dim(q_grouped, blk_start, REF_BLOCK, axis=1).astype(jnp.float32)
        scores = jnp.einsum("bqkgd,bskd->bkgqs", q_blk, k_f32) * att_scale
        query_pos = blk_start + jnp.arange(REF_BLOCK)
        allowed = key_pos[None, :] <= query_pos[:, None]
        scores = jnp.where(allowed, scores, -1e30)
        row_max = jnp.max(scores, axis=-1, keepdims=True)
        exp_f32 = jnp.exp(scores - row_max)
        row_sum = jnp.sum(exp_f32, axis=-1)
        weighted = jnp.einsum("bkgqs,bskd->bqkgd", exp_f32.astype(jnp.bfloat16).astype(jnp.float32), v_f32)
        return (weighted / jnp.transpose(row_sum, (0, 3, 1, 2))[..., None]).astype(jnp.bfloat16)

    blocks = lax.map(one_block, jnp.arange(n_blocks))
    return jnp.moveaxis(blocks, 0, 1).reshape(BATCH_SIZE, SEQ_LEN, N_HEADS, HEAD_DIM)


def transformer_layer(hidden, cos_t, sin_t, layer_weights):
    w_query, w_key, w_value, w_out, w_up, w_down, gain_attn, gain_mlp = layer_weights
    n_rows = BATCH_SIZE * SEQ_LEN
    normed = rms_norm(hidden, gain_attn).reshape(n_rows, D_MODEL)
    q_proj = jnp.dot(normed, w_query.reshape(D_MODEL, N_HEADS * HEAD_DIM), preferred_element_type=jnp.float32)
    k_proj = jnp.dot(normed, w_key.reshape(D_MODEL, N_KV_HEADS * HEAD_DIM), preferred_element_type=jnp.float32)
    v_proj = jnp.dot(normed, w_value.reshape(D_MODEL, N_KV_HEADS * HEAD_DIM), preferred_element_type=jnp.float32)
    q_heads = apply_rope(q_proj.reshape(BATCH_SIZE, SEQ_LEN, N_HEADS, HEAD_DIM), cos_t, sin_t)
    k_heads = apply_rope(k_proj.reshape(BATCH_SIZE, SEQ_LEN, N_KV_HEADS, HEAD_DIM), cos_t, sin_t)
    v_heads = v_proj.astype(jnp.bfloat16).reshape(BATCH_SIZE, SEQ_LEN, N_KV_HEADS, HEAD_DIM)
    attn_out = causal_attention(q_heads, k_heads, v_heads)
    attn_proj = jnp.dot(attn_out.reshape(n_rows, N_HEADS * HEAD_DIM), w_out.reshape(N_HEADS * HEAD_DIM, D_MODEL), preferred_element_type=jnp.float32)
    resid_h = (hidden.reshape(n_rows, D_MODEL).astype(jnp.float32) + attn_proj).astype(jnp.bfloat16)
    normed_mlp = rms_norm(resid_h, gain_mlp)
    gelu_act = jax.nn.gelu(jnp.dot(normed_mlp, w_up, preferred_element_type=jnp.float32), approximate=True).astype(jnp.bfloat16)
    layer_out = resid_h.astype(jnp.float32) + jnp.dot(gelu_act, w_down, preferred_element_type=jnp.float32)
    return layer_out.astype(jnp.bfloat16).reshape(BATCH_SIZE, SEQ_LEN, D_MODEL)


def reference(x_in, positions, w_query, w_key, w_value, w_out, w_up, w_down, g_attn, g_mlp):
    cos_t, sin_t = rope_tables(positions)

    def layer_body(hidden, layer_weights):
        return transformer_layer(hidden, cos_t, sin_t, layer_weights), None

    stacked = (w_query, w_key, w_value, w_out, w_up, w_down, g_attn, g_mlp)
    return lax.scan(layer_body, x_in, stacked)[0]
```

```python
import functools

import jax
import jax.numpy as jnp
from jax import lax
from jax.experimental import pallas as pl
from jax.experimental.pallas import tpu as pltpu
from jax.sharding import PartitionSpec as P

ROPE_BASE = 10000.0
NORM_EPS = 1e-6
N_CHUNKS = 2
BLK = 512
N_ROW_SLOTS = 5
N_UP_SLOTS = 3


def rope_tables(positions, head_dim):
    inv_freq = ROPE_BASE ** (-jnp.arange(head_dim // 2, dtype=jnp.float32) * (2.0 / head_dim))
    angles = positions.astype(jnp.float32)[..., None] * inv_freq
    return jnp.cos(angles), jnp.sin(angles)


def gelu(x):
    c = 0.7978845608028654
    return 0.5 * x * (1.0 + jnp.tanh(c * (x + 0.044715 * (x * x * x))))


def norm_rows(src_ref, gain, dst_ref, rows, step=64):
    def body(i, _):
        sl = pl.ds(pl.multiple_of(i * step, step), step)
        x = src_ref[sl, :].astype(jnp.float32)
        ms = jnp.mean(x * x, axis=-1, keepdims=True)
        dst_ref[sl, :] = (x * lax.rsqrt(ms + NORM_EPS) * gain).astype(jnp.bfloat16)
        return 0

    lax.fori_loop(0, rows // step, body, 0)


def dense_kernel(layer, with_mlp, with_qkv, rows, seq_loc, d_model, ff_dim, x_row, y_row, aliased, *refs):
    it = iter(refs)
    x_hbm = next(it)
    if with_mlp:
        o_hbm, wo_hbm, wu_hbm, wd_hbm, gm_ref = (next(it) for _ in range(5))
    if with_qkv:
        wq_hbm, wk_hbm, wv_hbm, ga_ref, tab_ref = (next(it) for _ in range(5))
    if aliased:
        next(it)
    if with_mlp:
        y_hbm = next(it)
    if with_qkv:
        q_hbm, kv_hbm = next(it), next(it)
    x_ref, n_ref, ring, ring_sem, x_sem, out_sem = (next(it) for _ in range(6))
    if with_mlp:
        o_ref, acc_ref, a_ref, up_ring, up_sem, o_sem = (next(it) for _ in range(6))
    if with_qkv:
        st_ref = next(it)

    n_o = d_model // BLK
    n_f = ff_dim // BLK
    n_q = d_model // BLK
    o_base = 0
    f_base = n_o if with_mlp else 0
    q_base = f_base + (n_f if with_mlp else 0)
    mlp_layer = layer - 1

    def start_o(j, slot):
        for i in range(4):
            for par in range(2):
                pltpu.make_async_copy(
                    wo_hbm.at[mlp_layer, j * 8 + par * 4 + i],
                    ring.at[slot, pl.ds((i * 2 + par) * 64, 64)],
                    ring_sem.at[slot],
                ).start()

    def start_down(f, slot):
        pltpu.make_async_copy(
            wd_hbm.at[mlp_layer, pl.ds(pl.multiple_of(f * BLK, BLK), BLK)], ring.at[slot], ring_sem.at[slot]
        ).start()

    def start_q(j, slot):
        for i in range(4):
            for half in range(2):
                for par in range(2):
                    pltpu.make_async_copy(
                        wq_hbm.at[layer, j * 8 + par * 4 + i, pl.ds(half * 32, 32)],
                        ring.at[slot, pl.ds(i * 128 + half * 64 + par * 32, 32)],
                        ring_sem.at[slot],
                    ).start()

    def start_k(slot):
        for gp in range(4):
            for half in range(2):
                for par in range(2):
                    pltpu.make_async_copy(
                        wk_hbm.at[layer, gp * 2 + par, pl.ds(half * 32, 32)],
                        ring.at[slot, pl.ds(gp * 128 + half * 64 + par * 32, 32)],
                        ring_sem.at[slot],
                    ).start()

    def start_v(slot):
        for g in range(8):
            pltpu.make_async_copy(wv_hbm.at[layer, g], ring.at[slot, pl.ds(g * 64, 64)], ring_sem.at[slot]).start()

    n_blocks = q_base + ((n_q + 2) if with_qkv else 0)

    def start_block(b):
        static = isinstance(b, int)
        slot = b % N_ROW_SLOTS if static else lax.rem(b, N_ROW_SLOTS)

        def guard(lo, hi, fn):
            if static:
                if lo <= b < hi:
                    fn()
            else:
                pl.when(jnp.logical_and(b >= lo, b < hi))(fn)

        if with_mlp:
            guard(o_base, f_base, lambda: start_o(b, slot))
            guard(f_base, q_base, lambda: start_down(b - f_base, slot))
        if with_qkv:
            guard(q_base, q_base + n_q, lambda: start_q(b - q_base, slot))
            guard(q_base + n_q, q_base + n_q + 1, lambda: start_k(slot))
            guard(q_base + n_q + 1, q_base + n_q + 2, lambda: start_v(slot))

    def wait_block(b):
        slot = b % N_ROW_SLOTS if isinstance(b, int) else lax.rem(b, N_ROW_SLOTS)
        pltpu.make_async_copy(ring.at[slot], ring.at[slot], ring_sem.at[slot]).wait()
        return slot

    def start_up(f):
        slot = f % N_UP_SLOTS if isinstance(f, int) else lax.rem(f, N_UP_SLOTS)
        pltpu.make_async_copy(
            wu_hbm.at[mlp_layer, :, pl.ds(pl.multiple_of(f * BLK, BLK), BLK)], up_ring.at[slot], up_sem.at[slot]
        ).start()

    def wait_up(f):
        slot = lax.rem(f, N_UP_SLOTS)
        pltpu.make_async_copy(up_ring.at[slot], up_ring.at[slot], up_sem.at[slot]).wait()
        return slot

    if with_mlp:
        for j in range(n_o):
            pltpu.make_async_copy(o_hbm.at[:, pl.ds(j * BLK, BLK)], o_ref.at[j], o_sem.at[j]).start()
            if j == 0:
                start_block(0)
    x_copy = pltpu.make_async_copy(x_hbm.at[pl.ds(x_row, rows)], x_ref, x_sem)
    x_copy.start()
    for b in range(1 if with_mlp else 0, N_ROW_SLOTS - 1):
        start_block(b)
    if with_mlp:
        for f in range(N_UP_SLOTS - 1):
            start_up(f)

    if with_mlp:
        def o_body(j, _):
            pltpu.make_async_copy(o_ref.at[j], o_ref.at[j], o_sem.at[j]).wait()
            slot = wait_block(j)
            start_block(j + N_ROW_SLOTS - 1)
            part = jnp.dot(o_ref[j], ring[slot], preferred_element_type=jnp.float32)

            @pl.when(j == 0)
            def _():
                acc_ref[...] = part

            @pl.when(j > 0)
            def _():
                acc_ref[...] += part

            return 0

        lax.fori_loop(0, n_o, o_body, 0)
        x_copy.wait()

        def resid_body(i, _):
            sl = pl.ds(pl.multiple_of(i * 64, 64), 64)
            h = (x_ref[sl, :].astype(jnp.float32) + acc_ref[sl, :]).astype(jnp.bfloat16)
            hf = h.astype(jnp.float32)
            ms = jnp.mean(hf * hf, axis=-1, keepdims=True)
            n_ref[sl, :] = (hf * lax.rsqrt(ms + NORM_EPS) * gm_ref[0]).astype(jnp.bfloat16)
            acc_ref[sl, :] = hf
            return 0

        lax.fori_loop(0, rows // 64, resid_body, 0)

        def up_part(f):
            slot = wait_up(f)

            @pl.when(f + N_UP_SLOTS - 1 < n_f)
            def _():
                start_up(f + N_UP_SLOTS - 1)

            u = jnp.dot(n_ref[...], up_ring[slot], preferred_element_type=jnp.float32)
            a_ref[lax.rem(f, 2)] = gelu(u).astype(jnp.bfloat16)

        def down_part(f):
            b = f_base + f
            slot = wait_block(b)
            start_block(b + N_ROW_SLOTS - 1)
            acc_ref[...] += jnp.dot(a_ref[lax.rem(f, 2)], ring[slot], preferred_element_type=jnp.float32)

        def f_body(f, _):
            up_part(f)
            down_part(f)
            return 0

        lax.fori_loop(0, n_f, f_body, 0)

        def y_body(i, _):
            sl = pl.ds(pl.multiple_of(i * 64, 64), 64)
            y = acc_ref[sl, :].astype(jnp.bfloat16)
            x_ref[sl, :] = y
            if with_qkv:
                yf = y.astype(jnp.float32)
                ms = jnp.mean(yf * yf, axis=-1, keepdims=True)
                n_ref[sl, :] = (yf * lax.rsqrt(ms + NORM_EPS) * ga_ref[0]).astype(jnp.bfloat16)
            return 0

        lax.fori_loop(0, rows // 64, y_body, 0)
        y_copy = pltpu.make_async_copy(x_ref, y_hbm.at[pl.ds(y_row, rows)], out_sem.at[0])
        y_copy.start()
    else:
        x_copy.wait()
        norm_rows(x_ref, ga_ref[0], n_ref, rows)

    if with_qkv:
        reps = rows // seq_loc

        def project(b):
            slot = wait_block(b)
            start_block(b + N_ROW_SLOTS - 1)
            return lax.dot_general(n_ref[...], ring[slot], (((1,), (1,)), ((), ())), preferred_element_type=jnp.float32)

        def rope(t, cos_t, sin_t):
            r3 = t.reshape(reps, seq_loc, 128)
            s3 = pltpu.roll(t, 64, 1).reshape(reps, seq_loc, 128)
            return (r3 * cos_t + s3 * sin_t).reshape(rows, 128).astype(jnp.bfloat16)

        def drain(s, dst):
            pltpu.make_async_copy(st_ref.at[s], dst, out_sem.at[1 + s]).wait()

        def q_body(j, _):
            s = lax.rem(j, 2)
            res = project(q_base + j)

            @pl.when(j >= 2)
            def _():
                drain(s, q_hbm.at[:, pl.ds(0, BLK)])

            for i in range(4):
                st_ref[s, :, i * 128 : (i + 1) * 128] = rope(res[:, i * 128 : (i + 1) * 128], tab_ref[0], tab_ref[1])
            pltpu.make_async_copy(
                st_ref.at[s], q_hbm.at[:, pl.ds(pl.multiple_of(j * BLK, BLK), BLK)], out_sem.at[1 + s]
            ).start()
            return 0

        lax.fori_loop(0, n_q, q_body, 0)
        kres = project(q_base + n_q)
        drain(0, q_hbm.at[:, pl.ds(0, BLK)])
        for i in range(4):
            st_ref[0, :, i * 128 : (i + 1) * 128] = rope(kres[:, i * 128 : (i + 1) * 128], tab_ref[2], tab_ref[3])
        pltpu.make_async_copy(st_ref.at[0], kv_hbm.at[:, pl.ds(0, BLK)], out_sem.at[1]).start()
        vres = project(q_base + n_q + 1)
        drain(1, q_hbm.at[:, pl.ds(0, BLK)])
        st_ref[1] = vres.astype(jnp.bfloat16)
        pltpu.make_async_copy(st_ref.at[1], kv_hbm.at[:, pl.ds(BLK, BLK)], out_sem.at[2]).start()
        drain(0, kv_hbm.at[:, pl.ds(0, BLK)])
        drain(1, kv_hbm.at[:, pl.ds(BLK, BLK)])
    if with_mlp:
        y_copy.wait()


def dense_call(layer, n_layers, x, x_row, rows, o, weights, tables, seq_loc, y_rows=None, y_row=0, y_into=None):
    w_query_t, w_key_t, w_value_t, w_out, w_up, w_down, g_attn, g_mlp = weights
    d_model = x.shape[1]
    ff_dim = w_up.shape[2]
    with_mlp = o is not None
    with_qkv = layer < n_layers
    any_spec = pl.BlockSpec(memory_space=pl.ANY)
    vmem_spec = pl.BlockSpec(memory_space=pltpu.VMEM)
    args, specs = [x], [any_spec]
    outs, out_specs = [], []
    flops = 0
    nbytes = 0
    if with_mlp:
        args += [o, w_out, w_up, w_down, g_mlp[layer - 1][None]]
        specs += [any_spec] * 4 + [vmem_spec]
        outs.append(jax.ShapeDtypeStruct((y_rows or rows, d_model), jnp.bfloat16))
        flops += 2 * rows * d_model * (d_model + 2 * ff_dim)
        nbytes += 2 * d_model * (d_model + 2 * ff_dim) + 6 * rows * d_model
    if with_qkv:
        args += [w_query_t, w_key_t, w_value_t, g_attn[layer][None], tables]
        specs += [any_spec] * 3 + [vmem_spec] * 2
        outs.append(jax.ShapeDtypeStruct((rows, d_model), jnp.bfloat16))
        outs.append(jax.ShapeDtypeStruct((rows, 2 * BLK), jnp.bfloat16))
        flops += 2 * rows * d_model * (d_model + 2 * BLK)
        nbytes += 2 * d_model * (d_model + 2 * BLK) + 5 * rows * d_model
    aliases = {}
    if y_into is not None:
        aliases = {len(args): 0}
        args.append(y_into)
        specs.append(any_spec)
    out_specs = [any_spec] * len(outs)
    scratch = [
        pltpu.VMEM((rows, d_model), jnp.bfloat16),
        pltpu.VMEM((rows, d_model), jnp.bfloat16),
        pltpu.VMEM((N_ROW_SLOTS, BLK, d_model), jnp.bfloat16),
        pltpu.SemaphoreType.DMA((N_ROW_SLOTS,)),
        pltpu.SemaphoreType.DMA,
        pltpu.SemaphoreType.DMA((3,)),
    ]
    if with_mlp:
        scratch += [
            pltpu.VMEM((d_model // BLK, rows, BLK), jnp.bfloat16),
            pltpu.VMEM((rows, d_model), jnp.float32),
            pltpu.VMEM((2, rows, BLK), jnp.bfloat16),
            pltpu.VMEM((N_UP_SLOTS, d_model, BLK), jnp.bfloat16),
            pltpu.SemaphoreType.DMA((N_UP_SLOTS,)),
            pltpu.SemaphoreType.DMA((d_model // BLK,)),
        ]
    if with_qkv:
        scratch.append(pltpu.VMEM((2, rows, BLK), jnp.bfloat16))
    return pl.pallas_call(
        functools.partial(
            dense_kernel, layer, with_mlp, with_qkv, rows, seq_loc, d_model, ff_dim, x_row, y_row, y_into is not None
        ),
        out_shape=outs,
        in_specs=specs,
        out_specs=out_specs,
        scratch_shapes=scratch,
        input_output_aliases=aliases,
        compiler_params=pltpu.CompilerParams(vmem_limit_bytes=60 * 1024 * 1024),
        cost_estimate=pl.CostEstimate(flops=flops, bytes_accessed=nbytes, transcendentals=0),
        name=f"dense_{int(with_mlp)}{int(with_qkv)}",
    )(*args)


def attn_kernel(n_dev, seq_loc, q_ref, kv_ref, bias_ref, o_ref):
    keys = n_dev * seq_loc
    lane = lax.broadcasted_iota(jnp.int32, (1, 128), 1)
    even = lax.rem(lane, 64) < 32
    first = lane < 64
    zero = jnp.zeros((), jnp.bfloat16)
    for gp in range(4):
        k_t = kv_ref[:, 0, :, gp * 128 : (gp + 1) * 128].reshape(keys, 128)
        v_t = kv_ref[:, 0, :, BLK + gp * 128 : BLK + (gp + 1) * 128].reshape(keys, 128)
        q_rows = []
        for i in range(4):
            c0 = gp * BLK + i * 128
            q_t = q_ref[0, :, c0 : c0 + 128]
            q_rows += [jnp.where(even, q_t, zero), jnp.where(even, zero, q_t)]
        q_s = jnp.concatenate(q_rows, axis=0)
        s = lax.dot_general(q_s, k_t, (((1,), (1,)), ((), ())), preferred_element_type=jnp.float32)
        s = (s.reshape(8, seq_loc, keys) + bias_ref[...][None]).reshape(8 * seq_loc, keys)
        m = jnp.max(s, axis=-1, keepdims=True)
        p = jnp.exp(s - m)
        l = jnp.sum(p, axis=-1, keepdims=True)
        acc = jnp.dot(p.astype(jnp.bfloat16), v_t, preferred_element_type=jnp.float32)
        o = (acc / l).reshape(4, 2, seq_loc, 128)
        for i in range(4):
            c0 = gp * BLK + i * 128
            o_ref[0, :, c0 : c0 + 128] = jnp.where(first, o[i, 0], o[i, 1]).astype(jnp.bfloat16)


def attn_call(q, kv, bias, seq_loc):
    rows, d_model = q.shape
    n_dev = kv.shape[0]
    n_b = rows // seq_loc
    keys = n_dev * seq_loc
    out = pl.pallas_call(
        functools.partial(attn_kernel, n_dev, seq_loc),
        grid=(n_b,),
        out_shape=jax.ShapeDtypeStruct((n_b, seq_loc, d_model), jnp.bfloat16),
        in_specs=[
            pl.BlockSpec((1, seq_loc, d_model), lambda b: (b, 0, 0)),
            pl.BlockSpec((n_dev, 1, seq_loc, 2 * BLK), lambda b: (0, b, 0, 0)),
            pl.BlockSpec((seq_loc, keys), lambda b: (0, 0)),
        ],
        out_specs=pl.BlockSpec((1, seq_loc, d_model), lambda b: (b, 0, 0)),
        compiler_params=pltpu.CompilerParams(
            dimension_semantics=("arbitrary",), vmem_limit_bytes=60 * 1024 * 1024
        ),
        cost_estimate=pl.CostEstimate(
            flops=16 * rows * d_model * keys, bytes_accessed=2 * kv.size + 4 * q.size, transcendentals=0
        ),
        name="attn",
    )(q.reshape(n_b, seq_loc, d_model), kv.reshape(n_dev, n_b, seq_loc, 2 * BLK), bias)
    return out.reshape(rows, d_model)


def solution(mesh):
    tok_spec = P(None, ("data", "seq"), None)
    in_specs = (tok_spec, P(("data", "seq"))) + (P(),) * 8

    def device_fn(x_loc, pos_loc, w_query, w_key, w_value, w_out, w_up, w_down, g_attn, g_mlp):
        n_batch, seq_loc, d_model = x_loc.shape
        n_layers = w_query.shape[0]
        n_dev = mesh.shape["seq"]
        scale = w_query.shape[-1] ** -0.5
        cos_t, sin_t = rope_tables(pos_loc, w_query.shape[-1])
        cos4 = jnp.concatenate([cos_t] * 4, axis=-1)
        sin4 = jnp.concatenate([-sin_t, -sin_t, sin_t, sin_t], axis=-1)
        tables = jnp.stack([cos4 * scale, sin4 * scale, cos4, sin4])
        me = lax.axis_index("seq")
        key_pos = jnp.arange(n_dev * seq_loc)
        query_pos = me * seq_loc + jnp.arange(seq_loc)
        bias = jnp.where(key_pos[None, :] <= query_pos[:, None], 0.0, -jnp.inf).astype(jnp.float32)
        weights = (
            jnp.transpose(w_query, (0, 2, 3, 1)),
            jnp.transpose(w_key, (0, 2, 3, 1)),
            jnp.transpose(w_value, (0, 2, 3, 1)),
            w_out,
            w_up,
            w_down,
            g_attn,
            g_mlp,
        )
        rows = n_batch // N_CHUNKS * seq_loc
        x_all = x_loc.reshape(n_batch * seq_loc, d_model)
        xs = [(x_all, c * rows) for c in range(N_CHUNKS)]
        qs, kvs = [None] * N_CHUNKS, [None] * N_CHUNKS
        for c in range(N_CHUNKS):
            qs[c], kv = dense_call(0, n_layers, *xs[c], rows, None, weights, tables, seq_loc)
            kvs[c] = lax.all_gather(kv, "seq", axis=0, tiled=False)
        out = None
        last = None
        for layer in range(1, n_layers + 1):
            for c in range(N_CHUNKS):
                if last is not None:
                    qs[c], _ = lax.optimization_barrier((qs[c], last))
                o = attn_call(qs[c], kvs[c], bias, seq_loc)
                if layer < n_layers:
                    y, qs[c], kv = dense_call(layer, n_layers, *xs[c], rows, o, weights, tables, seq_loc)
                    xs[c] = (y, 0)
                    kvs[c] = lax.all_gather(kv, "seq", axis=0, tiled=False)
                    last = y
                else:
                    (out,) = dense_call(
                        layer, n_layers, *xs[c], rows, o, weights, tables, seq_loc, n_batch * seq_loc, c * rows, out
                    )
                    last = out
        return out.reshape(n_batch, seq_loc, d_model)

    return jax.shard_map(device_fn, mesh=mesh, in_specs=in_specs, out_specs=tok_spec, check_vma=False)
```

```python
import functools

import jax
import jax.numpy as jnp
from jax import lax
from jax.experimental import pallas as pl
from jax.experimental.pallas import tpu as pltpu
from jax.sharding import PartitionSpec as P

ROPE_BASE = 10000.0
NORM_EPS = 1e-6
N_CHUNKS = 2
BLK = 512
N_ROW_SLOTS = 6
N_UP_SLOTS = 4
N_KV_SLOTS = 3
MASK_VALUE = -3.38e38


def rope_tables(positions, head_dim):
    inv_freq = ROPE_BASE ** (-jnp.arange(head_dim // 2, dtype=jnp.float32) * (2.0 / head_dim))
    angles = positions.astype(jnp.float32)[..., None] * inv_freq
    return jnp.cos(angles), jnp.sin(angles)


def gelu(x):
    c = 0.7978845608028654
    return 0.5 * x * (1.0 + jnp.tanh(c * (x + 0.044715 * (x * x * x))))


def norm_rows(src_ref, gain, dst_ref, rows, step=64):
    def body(i, _):
        sl = pl.ds(pl.multiple_of(i * step, step), step)
        x = src_ref[sl, :].astype(jnp.float32)
        ms = jnp.mean(x * x, axis=-1, keepdims=True)
        dst_ref[sl, :] = (x * lax.rsqrt(ms + NORM_EPS) * gain).astype(jnp.bfloat16)
        return 0

    lax.fori_loop(0, rows // step, body, 0)


def layer_kernel(layer, with_mlp, with_q, with_kv, rows, seq_loc, n_dev, d_model, ff_dim, x_row, y_row, aliased, *refs):
    with_qkv = with_q or with_kv
    it = iter(refs)
    x_hbm = next(it)
    if with_mlp:
        qin_hbm, kvin_hbm, mask_ref, wo_hbm, wu_hbm, wd_hbm, gm_ref = (next(it) for _ in range(7))
    if with_qkv:
        wq_hbm, wk_hbm, wv_hbm, ga_ref, tab_ref = (next(it) for _ in range(5))
    if aliased:
        next(it)
    if with_mlp:
        y_hbm = next(it)
    if with_q:
        q_hbm = next(it)
    if with_kv:
        kv_hbm = next(it)
    x_ref, n_ref, ring, ring_sem, x_sem, out_sem = (next(it) for _ in range(6))
    if with_mlp:
        o_ref, acc_ref, u_ref, a_ref, up_ring, up_sem, q_ref, q_sem, kv_ring, kv_sem = (next(it) for _ in range(10))
    if with_qkv:
        st_ref = next(it)

    n_o = d_model // BLK
    n_f = ff_dim // BLK
    n_q = d_model // BLK if with_q else 0
    n_kv = 2 if with_kv else 0
    o_base = 0
    f_base = n_o if with_mlp else 0
    q_base = f_base + (n_f if with_mlp else 0)
    mlp_layer = layer - 1

    def start_o(j, slot):
        for i in range(4):
            for par in range(2):
                pltpu.make_async_copy(
                    wo_hbm.at[mlp_layer, j * 8 + par * 4 + i],
                    ring.at[slot, pl.ds((i * 2 + par) * 64, 64)],
                    ring_sem.at[slot],
                ).start()

    def start_down(f, slot):
        for z in range(4):
            row = f * BLK + z * 128
            pltpu.make_async_copy(
                wd_hbm.at[mlp_layer, pl.ds(row if isinstance(f, int) else pl.multiple_of(row, 128), 128)],
                ring.at[slot, pl.ds(z * 128, 128)],
                ring_sem.at[slot],
            ).start()

    def start_q(j, slot):
        for i in range(4):
            for half in range(2):
                for par in range(2):
                    pltpu.make_async_copy(
                        wq_hbm.at[layer, j * 8 + par * 4 + i, pl.ds(half * 32, 32)],
                        ring.at[slot, pl.ds(i * 128 + half * 64 + par * 32, 32)],
                        ring_sem.at[slot],
                    ).start()

    def start_k(slot):
        for gp in range(4):
            for half in range(2):
                for par in range(2):
                    pltpu.make_async_copy(
                        wk_hbm.at[layer, gp * 2 + par, pl.ds(half * 32, 32)],
                        ring.at[slot, pl.ds(gp * 128 + half * 64 + par * 32, 32)],
                        ring_sem.at[slot],
                    ).start()

    def start_v(slot):
        for g in range(8):
            pltpu.make_async_copy(wv_hbm.at[layer, g], ring.at[slot, pl.ds(g * 64, 64)], ring_sem.at[slot]).start()

    n_blocks = q_base + n_q + n_kv

    def start_block(b):
        static = isinstance(b, int)
        slot = b % N_ROW_SLOTS if static else lax.rem(b, N_ROW_SLOTS)

        def guard(lo, hi, fn):
            if static:
                if lo <= b < hi:
                    fn()
            else:
                pl.when(jnp.logical_and(b >= lo, b < hi))(fn)

        if with_mlp:
            guard(o_base, f_base, lambda: start_o(b, slot))
            guard(f_base, q_base, lambda: start_down(b - f_base, slot))
        if with_q:
            guard(q_base, q_base + n_q, lambda: start_q(b - q_base, slot))
        if with_kv:
            guard(q_base + n_q, q_base + n_q + 1, lambda: start_k(slot))
            guard(q_base + n_q + 1, q_base + n_q + 2, lambda: start_v(slot))

    def wait_block(b):
        slot = b % N_ROW_SLOTS if isinstance(b, int) else lax.rem(b, N_ROW_SLOTS)
        pltpu.make_async_copy(ring.at[slot], ring.at[slot], ring_sem.at[slot]).wait()
        return slot

    def start_up(f):
        slot = f % N_UP_SLOTS if isinstance(f, int) else lax.rem(f, N_UP_SLOTS)
        col = f * BLK if isinstance(f, int) else pl.multiple_of(f * BLK, BLK)
        for z in range(4):
            pltpu.make_async_copy(
                wu_hbm.at[mlp_layer, pl.ds(z * BLK, BLK), pl.ds(col, BLK)],
                up_ring.at[slot, pl.ds(z * BLK, BLK)],
                up_sem.at[slot],
            ).start()

    def wait_up(f):
        slot = f % N_UP_SLOTS if isinstance(f, int) else lax.rem(f, N_UP_SLOTS)
        pltpu.make_async_copy(up_ring.at[slot], up_ring.at[slot], up_sem.at[slot]).wait()
        return slot

    n_b = rows // seq_loc

    def start_kv(i):
        slot = i % N_KV_SLOTS if isinstance(i, int) else lax.rem(i, N_KV_SLOTS)
        row = i * seq_loc if isinstance(i, int) else pl.multiple_of(i * seq_loc, seq_loc)
        pltpu.make_async_copy(kvin_hbm.at[:, pl.ds(row, seq_loc)], kv_ring.at[slot], kv_sem.at[slot]).start()

    x_copy = pltpu.make_async_copy(x_hbm.at[pl.ds(x_row, rows)], x_ref, x_sem)
    if with_mlp:
        q_copy = pltpu.make_async_copy(qin_hbm, q_ref, q_sem)
        q_copy.start()
        for i in range(N_KV_SLOTS - 1):
            start_kv(i)
    x_copy.start()
    for b in range(min(N_ROW_SLOTS - 1, n_blocks)):
        start_block(b)
    if with_mlp:
        for f in range(N_UP_SLOTS):
            start_up(f)

    if with_mlp:
        keys = n_dev * seq_loc
        lane = lax.broadcasted_iota(jnp.int32, (1, 128), 1)
        even = lax.rem(lane, 64) < 32
        first = lane < 64
        zero = jnp.zeros((), jnp.bfloat16)
        eye = jnp.where(
            lax.broadcasted_iota(jnp.int32, (seq_loc, 128), 0) == lax.broadcasted_iota(jnp.int32, (seq_loc, 128), 1), 1.0, 0.0
        ).astype(jnp.bfloat16)
        q_copy.wait()

        def attn_body(i, _):
            slot = lax.rem(i, N_KV_SLOTS)
            pltpu.make_async_copy(kv_ring.at[slot], kv_ring.at[slot], kv_sem.at[slot]).wait()

            @pl.when(i + N_KV_SLOTS - 1 < n_b)
            def _():
                start_kv(i + N_KV_SLOTS - 1)

            sl = pl.ds(pl.multiple_of(i * seq_loc, seq_loc), seq_loc)
            for gp in range(4):
                k_t = kv_ring[slot, :, :, gp * 128 : (gp + 1) * 128].reshape(keys, 128)
                v_t = kv_ring[slot, :, :, BLK + gp * 128 : BLK + (gp + 1) * 128].reshape(keys, 128)
                k_ext = jnp.concatenate([k_t, mask_ref[...]], axis=1)
                q_rows = []
                for h in range(4):
                    c0 = gp * BLK + h * 128
                    q_t = q_ref[sl, c0 : c0 + 128]
                    q_rows.append(jnp.concatenate([jnp.where(even, q_t, zero), eye], axis=1))
                    q_rows.append(jnp.concatenate([jnp.where(even, zero, q_t), eye], axis=1))
                s = lax.dot_general(
                    jnp.concatenate(q_rows, axis=0), k_ext, (((1,), (1,)), ((), ())), preferred_element_type=jnp.float32
                )
                m = jnp.max(s, axis=-1, keepdims=True)
                p = jnp.exp(s - m)
                l = jnp.sum(p, axis=-1, keepdims=True)
                o = jnp.dot(p.astype(jnp.bfloat16), v_t, preferred_element_type=jnp.float32)
                o = (o / l).reshape(4, 2, seq_loc, 128)
                for h in range(4):
                    o_ref[gp, sl, h * 128 : (h + 1) * 128] = jnp.where(first, o[h, 0], o[h, 1]).astype(jnp.bfloat16)
            return 0

        lax.fori_loop(0, n_b, attn_body, 0)

        def o_part(j):
            slot = wait_block(j)
            if isinstance(j, int):
                start_block(j + N_ROW_SLOTS - 1)
            else:
                pl.when(j < n_o - 1)(lambda: start_block(j + N_ROW_SLOTS - 1))
            return jnp.dot(o_ref[j], ring[slot], preferred_element_type=jnp.float32)

        acc_ref[...] = o_part(0)

        def o_body(j, _):
            acc_ref[...] += o_part(j)
            return 0

        lax.fori_loop(1, n_o, o_body, 0)
        x_copy.wait()

        def resid_body(i, _):
            sl = pl.ds(pl.multiple_of(i * 64, 64), 64)
            h = (x_ref[sl, :].astype(jnp.float32) + acc_ref[sl, :]).astype(jnp.bfloat16)
            hf = h.astype(jnp.float32)
            ms = jnp.mean(hf * hf, axis=-1, keepdims=True)
            n_ref[sl, :] = (hf * lax.rsqrt(ms + NORM_EPS) * gm_ref[0]).astype(jnp.bfloat16)
            acc_ref[sl, :] = hf
            return 0

        lax.fori_loop(0, rows // 64, resid_body, 0)

        def up_part(slot):
            u_ref[...] = jnp.dot(n_ref[...], up_ring[slot], preferred_element_type=jnp.float32)

        def gelu_part(s):
            a_ref[s] = gelu(u_ref[...]).astype(jnp.bfloat16)

        def down_part(slot, s):
            acc_ref[...] += jnp.dot(a_ref[s], ring[slot], preferred_element_type=jnp.float32)

        def next_down(f):
            slots = [wait_block(f_base + f + s) for s in range(2)]
            for s in range(2):
                start_block(f_base + f + s + N_ROW_SLOTS - 2)
            return slots

        ups = [wait_up(0), wait_up(1)]
        up_part(ups[0])
        gelu_part(0)
        up_part(ups[1])

        def f_body(g, _):
            downs = next_down(2 * g)
            ups = [wait_up(2 * g + 2 + s) for s in range(2)]
            for s in range(2):
                nxt = 2 * g + N_UP_SLOTS + s
                pl.when(nxt < n_f)(functools.partial(start_up, nxt))
            for s in range(2):
                gelu_part(1 - s)
                down_part(downs[s], s)
                up_part(ups[s])
            return 0

        lax.fori_loop(0, n_f // 2 - 1, f_body, 0)
        downs = next_down(n_f - 2)
        gelu_part(1)
        down_part(downs[0], 0)
        down_part(downs[1], 1)
        start_block(q_base + N_ROW_SLOTS - 2)

        def y_body(i, _):
            sl = pl.ds(pl.multiple_of(i * 64, 64), 64)
            y = acc_ref[sl, :].astype(jnp.bfloat16)
            x_ref[sl, :] = y
            if with_qkv:
                yf = y.astype(jnp.float32)
                ms = jnp.mean(yf * yf, axis=-1, keepdims=True)
                n_ref[sl, :] = (yf * lax.rsqrt(ms + NORM_EPS) * ga_ref[0]).astype(jnp.bfloat16)
            return 0

        lax.fori_loop(0, rows // 64, y_body, 0)
        y_copy = pltpu.make_async_copy(x_ref, y_hbm.at[pl.ds(y_row, rows)], out_sem.at[0])
        y_copy.start()
    else:
        x_copy.wait()
        norm_rows(x_ref, ga_ref[0], n_ref, rows)

    if with_qkv:
        reps = rows // seq_loc

        def project(b):
            slot = wait_block(b)
            start_block(b + N_ROW_SLOTS - 1)
            return lax.dot_general(n_ref[...], ring[slot], (((1,), (1,)), ((), ())), preferred_element_type=jnp.float32)

        def rope(t, cos_t, sin_t):
            r3 = t.reshape(reps, seq_loc, 128)
            s3 = pltpu.roll(t, 64, 1).reshape(reps, seq_loc, 128)
            return (r3 * cos_t + s3 * sin_t).reshape(rows, 128).astype(jnp.bfloat16)

        def drain(s, dst):
            pltpu.make_async_copy(st_ref.at[s], dst, out_sem.at[1 + s]).wait()

        def q_body(j, _):
            s = lax.rem(j, 2)

            @pl.when(j >= 2)
            def _():
                drain(s, q_hbm.at[:, pl.ds(0, BLK)])

            res = project(q_base + j)
            for i in range(4):
                st_ref[s, :, i * 128 : (i + 1) * 128] = rope(res[:, i * 128 : (i + 1) * 128], tab_ref[0], tab_ref[1])
            pltpu.make_async_copy(
                st_ref.at[s], q_hbm.at[:, pl.ds(pl.multiple_of(j * BLK, BLK), BLK)], out_sem.at[1 + s]
            ).start()
            return 0

        if with_q:
            lax.fori_loop(0, n_q, q_body, 0)
        if with_kv:
            if with_q:
                drain(0, q_hbm.at[:, pl.ds(0, BLK)])
            kres = project(q_base + n_q)
            for i in range(4):
                st_ref[0, :, i * 128 : (i + 1) * 128] = rope(kres[:, i * 128 : (i + 1) * 128], tab_ref[2], tab_ref[3])
            pltpu.make_async_copy(st_ref.at[0], kv_hbm.at[:, pl.ds(0, BLK)], out_sem.at[1]).start()
            if with_q:
                drain(1, q_hbm.at[:, pl.ds(0, BLK)])
            vres = project(q_base + n_q + 1)
            st_ref[1] = vres.astype(jnp.bfloat16)
            pltpu.make_async_copy(st_ref.at[1], kv_hbm.at[:, pl.ds(BLK, BLK)], out_sem.at[2]).start()
            drain(0, kv_hbm.at[:, pl.ds(0, BLK)])
            drain(1, kv_hbm.at[:, pl.ds(BLK, BLK)])
        else:
            drain(0, q_hbm.at[:, pl.ds(0, BLK)])
            drain(1, q_hbm.at[:, pl.ds(0, BLK)])
    if with_mlp:
        y_copy.wait()


def layer_call(
    layer, x, x_row, rows, attn_in, weights, tables, seq_loc, n_dev, with_q, with_kv, y_rows=None, y_row=0, y_into=None
):
    w_query_t, w_key_t, w_value_t, w_out, w_up, w_down, g_attn, g_mlp = weights
    d_model = x.shape[1]
    ff_dim = w_up.shape[2]
    with_mlp = attn_in is not None
    any_spec = pl.BlockSpec(memory_space=pl.ANY)
    vmem_spec = pl.BlockSpec(memory_space=pltpu.VMEM)
    args, specs = [x], [any_spec]
    outs = []
    flops = 0
    nbytes = 0
    if with_mlp:
        q, kv, mask = attn_in
        args += [q, kv, mask, w_out, w_up, w_down, g_mlp[layer - 1][None]]
        specs += [any_spec] * 2 + [vmem_spec] + [any_spec] * 3 + [vmem_spec]
        outs.append(jax.ShapeDtypeStruct((y_rows or rows, d_model), jnp.bfloat16))
        flops += 2 * rows * d_model * (d_model + 2 * ff_dim) + 16 * rows * d_model * n_dev * seq_loc
        nbytes += 2 * d_model * (d_model + 2 * ff_dim) + 6 * rows * d_model + 2 * kv.size
    if with_q or with_kv:
        args += [w_query_t, w_key_t, w_value_t, g_attn[layer][None], tables]
        specs += [any_spec] * 3 + [vmem_spec] * 2
        n_out = (d_model if with_q else 0) + (2 * BLK if with_kv else 0)
        flops += 2 * rows * d_model * n_out
        nbytes += 2 * d_model * n_out + 2 * rows * n_out
    if with_q:
        outs.append(jax.ShapeDtypeStruct((rows, d_model), jnp.bfloat16))
    if with_kv:
        outs.append(jax.ShapeDtypeStruct((rows, 2 * BLK), jnp.bfloat16))
    aliases = {}
    if y_into is not None:
        aliases = {len(args): 0}
        args.append(y_into)
        specs.append(any_spec)
    scratch = [
        pltpu.VMEM((rows, d_model), jnp.bfloat16),
        pltpu.VMEM((rows, d_model), jnp.bfloat16),
        pltpu.VMEM((N_ROW_SLOTS, BLK, d_model), jnp.bfloat16),
        pltpu.SemaphoreType.DMA((N_ROW_SLOTS,)),
        pltpu.SemaphoreType.DMA,
        pltpu.SemaphoreType.DMA((3,)),
    ]
    if with_mlp:
        scratch += [
            pltpu.VMEM((d_model // BLK, rows, BLK), jnp.bfloat16),
            pltpu.VMEM((rows, d_model), jnp.float32),
            pltpu.VMEM((rows, BLK), jnp.float32),
            pltpu.VMEM((2, rows, BLK), jnp.bfloat16),
            pltpu.VMEM((N_UP_SLOTS, d_model, BLK), jnp.bfloat16),
            pltpu.SemaphoreType.DMA((N_UP_SLOTS,)),
            pltpu.VMEM((rows, d_model), jnp.bfloat16),
            pltpu.SemaphoreType.DMA,
            pltpu.VMEM((N_KV_SLOTS, n_dev, seq_loc, 2 * BLK), jnp.bfloat16),
            pltpu.SemaphoreType.DMA((N_KV_SLOTS,)),
        ]
    if with_q or with_kv:
        scratch.append(pltpu.VMEM((2, rows, BLK), jnp.bfloat16))
    return pl.pallas_call(
        functools.partial(
            layer_kernel, layer, with_mlp, with_q, with_kv, rows, seq_loc, n_dev, d_model, ff_dim, x_row, y_row,
            y_into is not None,
        ),
        out_shape=outs,
        in_specs=specs,
        out_specs=[any_spec] * len(outs),
        scratch_shapes=scratch,
        input_output_aliases=aliases,
        compiler_params=pltpu.CompilerParams(vmem_limit_bytes=60 * 1024 * 1024),
        cost_estimate=pl.CostEstimate(flops=flops, bytes_accessed=nbytes, transcendentals=0),
        name=f"layer_{int(with_mlp)}{int(with_q)}{int(with_kv)}",
    )(*args)


def solution(mesh):
    tok_spec = P(None, ("data", "seq"), None)
    in_specs = (tok_spec, P(("data", "seq"))) + (P(),) * 8

    def device_fn(x_loc, pos_loc, w_query, w_key, w_value, w_out, w_up, w_down, g_attn, g_mlp):
        n_batch, seq_loc, d_model = x_loc.shape
        n_layers = w_query.shape[0]
        n_dev = mesh.shape["seq"]
        scale = w_query.shape[-1] ** -0.5
        cos_t, sin_t = rope_tables(pos_loc, w_query.shape[-1])
        cos4 = jnp.concatenate([cos_t] * 4, axis=-1)
        sin4 = jnp.concatenate([-sin_t, -sin_t, sin_t, sin_t], axis=-1)
        tables = jnp.stack([cos4 * scale, sin4 * scale, cos4, sin4])
        me = lax.axis_index("seq")
        key_pos = jnp.arange(n_dev * seq_loc)
        query_pos = me * seq_loc + jnp.arange(seq_loc)
        mask = jnp.where(key_pos[:, None] <= query_pos[None, :], 0.0, MASK_VALUE)
        mask = jnp.pad(mask, ((0, 0), (0, 128 - seq_loc))).astype(jnp.bfloat16)
        weights = (
            jnp.transpose(w_query, (0, 2, 3, 1)),
            jnp.transpose(w_key, (0, 2, 3, 1)),
            jnp.transpose(w_value, (0, 2, 3, 1)),
            w_out,
            w_up,
            w_down,
            g_attn,
            g_mlp,
        )
        rows = n_batch // N_CHUNKS * seq_loc
        x_all = x_loc.reshape(n_batch * seq_loc, d_model)
        xs = [(x_all, c * rows) for c in range(N_CHUNKS)]
        qs, kvs = [None] * N_CHUNKS, [None] * N_CHUNKS
        call = functools.partial(layer_call, weights=weights, tables=tables, seq_loc=seq_loc, n_dev=n_dev, rows=rows)
        last = None
        for c in range(N_CHUNKS):
            x_c = x_all
            if last is not None:
                x_c, _ = lax.optimization_barrier((x_all, last))
            (kv,) = call(0, x_c, c * rows, attn_in=None, with_q=False, with_kv=True)
            kvs[c] = lax.all_gather(kv, "seq", axis=0, tiled=False)
            last = kv
        for c in range(N_CHUNKS):
            x_c, _ = lax.optimization_barrier((x_all, last))
            (qs[c],) = call(0, x_c, c * rows, attn_in=None, with_q=True, with_kv=False)
            last = qs[c]
        out = None
        for layer in range(1, n_layers + 1):
            for c in range(N_CHUNKS):
                q_c, last = lax.optimization_barrier((qs[c], last))
                attn_in = (q_c, kvs[c], mask)
                if layer < n_layers:
                    y, qs[c], kv = call(layer, *xs[c], attn_in=attn_in, with_q=True, with_kv=True)
                    xs[c] = (y, 0)
                    kvs[c] = lax.all_gather(kv, "seq", axis=0, tiled=False)
                    last = y
                else:
                    (out,) = call(
                        layer, *xs[c], attn_in=attn_in, with_q=False, with_kv=False,
                        y_rows=n_batch * seq_loc, y_row=c * rows, y_into=out,
                    )
                    last = out
        return out.reshape(n_batch, seq_loc, d_model)

    return jax.shard_map(device_fn, mesh=mesh, in_specs=in_specs, out_specs=tok_spec, check_vma=False)
```

```python
import functools

import jax
import jax.numpy as jnp
from jax import lax
from jax.experimental import pallas as pl
from jax.experimental.pallas import tpu as pltpu
from jax.sharding import PartitionSpec as P

ROPE_BASE = 10000.0
NORM_EPS = 1e-6
N_CHUNKS = 2
BLK = 512
N_ROW_SLOTS = 6
N_UP_SLOTS = 4
N_KV_SLOTS = 3
MASK_VALUE = -3.38e38


def rope_tables(positions, head_dim):
    inv_freq = ROPE_BASE ** (-jnp.arange(head_dim // 2, dtype=jnp.float32) * (2.0 / head_dim))
    angles = positions.astype(jnp.float32)[..., None] * inv_freq
    return jnp.cos(angles), jnp.sin(angles)


def gelu(x):
    c = 0.7978845608028654
    return 0.5 * x * (1.0 + jnp.tanh(c * (x + 0.044715 * (x * x * x))))


def norm_rows(src_ref, gain, dst_ref, rows, step=64):
    def body(i, _):
        sl = pl.ds(pl.multiple_of(i * step, step), step)
        x = src_ref[sl, :].astype(jnp.float32)
        ms = jnp.mean(x * x, axis=-1, keepdims=True)
        dst_ref[sl, :] = (x * lax.rsqrt(ms + NORM_EPS) * gain).astype(jnp.bfloat16)
        return 0

    lax.fori_loop(0, rows // step, body, 0)


def layer_kernel(layer, with_mlp, with_q, with_kv, rows, seq_loc, n_dev, d_model, ff_dim, x_row, y_row, aliased, *refs):
    with_qkv = with_q or with_kv
    it = iter(refs)
    x_hbm = next(it)
    if with_mlp:
        qin_hbm, kvin_hbm, mask_ref, wo_hbm, wu_hbm, wd_hbm, gm_ref = (next(it) for _ in range(7))
    if with_qkv:
        wq_hbm, wk_hbm, wv_hbm, ga_ref, tab_ref = (next(it) for _ in range(5))
    if aliased:
        next(it)
    if with_mlp:
        y_hbm = next(it)
    if with_q:
        q_hbm = next(it)
    if with_kv:
        kv_hbm = next(it)
    x_ref, n_ref, ring, ring_sem, x_sem, out_sem = (next(it) for _ in range(6))
    if with_mlp:
        o_ref, acc_ref, u_ref, a_ref, up_ring, up_sem, q_ref, q_sem, kv_ring, kv_sem = (next(it) for _ in range(10))
    if with_qkv:
        st_ref = next(it)

    n_o = d_model // BLK
    n_f = ff_dim // BLK
    n_q = d_model // BLK if with_q else 0
    n_kv = 2 if with_kv else 0
    o_base = 0
    f_base = n_o if with_mlp else 0
    q_base = f_base + (n_f if with_mlp else 0)
    mlp_layer = layer - 1

    def start_o(j, slot):
        for i in range(4):
            for par in range(2):
                pltpu.make_async_copy(
                    wo_hbm.at[mlp_layer, j * 8 + par * 4 + i],
                    ring.at[slot, pl.ds((i * 2 + par) * 64, 64)],
                    ring_sem.at[slot],
                ).start()

    def start_down(f, slot):
        for z in range(4):
            row = f * BLK + z * 128
            pltpu.make_async_copy(
                wd_hbm.at[mlp_layer, pl.ds(row if isinstance(f, int) else pl.multiple_of(row, 128), 128)],
                ring.at[slot, pl.ds(z * 128, 128)],
                ring_sem.at[slot],
            ).start()

    def start_q(j, slot):
        for i in range(4):
            for half in range(2):
                for par in range(2):
                    pltpu.make_async_copy(
                        wq_hbm.at[layer, j * 8 + par * 4 + i, pl.ds(half * 32, 32)],
                        ring.at[slot, pl.ds(i * 128 + half * 64 + par * 32, 32)],
                        ring_sem.at[slot],
                    ).start()

    def start_k(slot):
        for gp in range(4):
            for half in range(2):
                for par in range(2):
                    pltpu.make_async_copy(
                        wk_hbm.at[layer, gp * 2 + par, pl.ds(half * 32, 32)],
                        ring.at[slot, pl.ds(gp * 128 + half * 64 + par * 32, 32)],
                        ring_sem.at[slot],
                    ).start()

    def start_v(slot):
        for g in range(8):
            pltpu.make_async_copy(wv_hbm.at[layer, g], ring.at[slot, pl.ds(g * 64, 64)], ring_sem.at[slot]).start()

    n_blocks = q_base + n_q + n_kv

    def start_block(b):
        static = isinstance(b, int)
        slot = b % N_ROW_SLOTS if static else lax.rem(b, N_ROW_SLOTS)

        def guard(lo, hi, fn):
            if static:
                if lo <= b < hi:
                    fn()
            else:
                pl.when(jnp.logical_and(b >= lo, b < hi))(fn)

        if with_mlp:
            guard(o_base, f_base, lambda: start_o(b, slot))
            guard(f_base, q_base, lambda: start_down(b - f_base, slot))
        if with_q:
            guard(q_base, q_base + n_q, lambda: start_q(b - q_base, slot))
        if with_kv:
            guard(q_base + n_q, q_base + n_q + 1, lambda: start_k(slot))
            guard(q_base + n_q + 1, q_base + n_q + 2, lambda: start_v(slot))

    def wait_block(b):
        slot = b % N_ROW_SLOTS if isinstance(b, int) else lax.rem(b, N_ROW_SLOTS)
        pltpu.make_async_copy(ring.at[slot], ring.at[slot], ring_sem.at[slot]).wait()
        return slot

    def start_up(f):
        slot = f % N_UP_SLOTS if isinstance(f, int) else lax.rem(f, N_UP_SLOTS)
        col = f * BLK if isinstance(f, int) else pl.multiple_of(f * BLK, BLK)
        for z in range(4):
            pltpu.make_async_copy(
                wu_hbm.at[mlp_layer, pl.ds(z * BLK, BLK), pl.ds(col, BLK)],
                up_ring.at[slot, pl.ds(z * BLK, BLK)],
                up_sem.at[slot],
            ).start()

    def wait_up(f):
        slot = f % N_UP_SLOTS if isinstance(f, int) else lax.rem(f, N_UP_SLOTS)
        pltpu.make_async_copy(up_ring.at[slot], up_ring.at[slot], up_sem.at[slot]).wait()
        return slot

    n_b = rows // seq_loc

    def start_kv(i):
        slot = i % N_KV_SLOTS if isinstance(i, int) else lax.rem(i, N_KV_SLOTS)
        row = i * seq_loc if isinstance(i, int) else pl.multiple_of(i * seq_loc, seq_loc)
        pltpu.make_async_copy(kvin_hbm.at[:, pl.ds(row, seq_loc)], kv_ring.at[slot], kv_sem.at[slot]).start()

    x_copy = pltpu.make_async_copy(x_hbm.at[pl.ds(x_row, rows)], x_ref, x_sem)
    if with_mlp:
        q_copy = pltpu.make_async_copy(qin_hbm, q_ref, q_sem)
        q_copy.start()
        for i in range(N_KV_SLOTS - 1):
            start_kv(i)
    if not with_mlp:
        x_copy.start()
        for b in range(min(N_ROW_SLOTS - 1, n_blocks)):
            start_block(b)

    if with_mlp:
        keys = n_dev * seq_loc
        lane = lax.broadcasted_iota(jnp.int32, (1, 128), 1)
        even = lax.rem(lane, 64) < 32
        first = lane < 64
        zero = jnp.zeros((), jnp.bfloat16)
        eye = jnp.where(
            lax.broadcasted_iota(jnp.int32, (seq_loc, 128), 0) == lax.broadcasted_iota(jnp.int32, (seq_loc, 128), 1), 1.0, 0.0
        ).astype(jnp.bfloat16)
        q_copy.wait()

        def attn_body(i, _):
            slot = lax.rem(i, N_KV_SLOTS)
            pltpu.make_async_copy(kv_ring.at[slot], kv_ring.at[slot], kv_sem.at[slot]).wait()

            @pl.when(i + N_KV_SLOTS - 1 < n_b)
            def _():
                start_kv(i + N_KV_SLOTS - 1)

            pl.when(i == 0)(x_copy.start)
            pl.when(jnp.logical_and(i >= 1, i < N_ROW_SLOTS))(lambda: start_block(i - 1))
            pl.when(i >= n_b - N_UP_SLOTS)(lambda: start_up(i - (n_b - N_UP_SLOTS)))

            sl = pl.ds(pl.multiple_of(i * seq_loc, seq_loc), seq_loc)
            for gp in range(4):
                k_t = kv_ring[slot, :, :, gp * 128 : (gp + 1) * 128].reshape(keys, 128)
                v_t = kv_ring[slot, :, :, BLK + gp * 128 : BLK + (gp + 1) * 128].reshape(keys, 128)
                k_ext = jnp.concatenate([k_t, mask_ref[...]], axis=1)
                q_rows = []
                for h in range(4):
                    c0 = gp * BLK + h * 128
                    q_t = q_ref[sl, c0 : c0 + 128]
                    q_rows.append(jnp.concatenate([jnp.where(even, q_t, zero), eye], axis=1))
                    q_rows.append(jnp.concatenate([jnp.where(even, zero, q_t), eye], axis=1))
                s = lax.dot_general(
                    jnp.concatenate(q_rows, axis=0), k_ext, (((1,), (1,)), ((), ())), preferred_element_type=jnp.float32
                )
                m = jnp.max(s, axis=-1, keepdims=True)
                p = jnp.exp(s - m)
                l = jnp.sum(p, axis=-1, keepdims=True)
                o = jnp.dot(p.astype(jnp.bfloat16), v_t, preferred_element_type=jnp.float32)
                o = (o / l).reshape(4, 2, seq_loc, 128)
                for h in range(4):
                    o_ref[gp, sl, h * 128 : (h + 1) * 128] = jnp.where(first, o[h, 0], o[h, 1]).astype(jnp.bfloat16)
            return 0

        lax.fori_loop(0, n_b, attn_body, 0)

        def o_part(j):
            slot = wait_block(j)
            if isinstance(j, int):
                start_block(j + N_ROW_SLOTS - 1)
            else:
                pl.when(j < n_o - 1)(lambda: start_block(j + N_ROW_SLOTS - 1))
            return jnp.dot(o_ref[j], ring[slot], preferred_element_type=jnp.float32)

        acc_ref[...] = o_part(0)

        def o_body(j, _):
            part = o_part(j)
            acc_ref[...] += part
            return 0

        lax.fori_loop(1, n_o, o_body, 0)
        x_copy.wait()

        def resid_body(i, _):
            sl = pl.ds(pl.multiple_of(i * 64, 64), 64)
            h = (x_ref[sl, :].astype(jnp.float32) + acc_ref[sl, :]).astype(jnp.bfloat16)
            hf = h.astype(jnp.float32)
            ms = jnp.mean(hf * hf, axis=-1, keepdims=True)
            n_ref[sl, :] = (hf * lax.rsqrt(ms + NORM_EPS) * gm_ref[mlp_layer]).astype(jnp.bfloat16)
            acc_ref[sl, :] = hf
            return 0

        lax.fori_loop(0, rows // 64, resid_body, 0)

        def up_part(slot):
            u_ref[...] = jnp.dot(n_ref[...], up_ring[slot], preferred_element_type=jnp.float32)

        def gelu_part(s):
            a_ref[s] = gelu(u_ref[...]).astype(jnp.bfloat16)

        def down_part(slot, s):
            acc_ref[...] += jnp.dot(a_ref[s], ring[slot], preferred_element_type=jnp.float32)

        def next_down(f):
            slots = [wait_block(f_base + f + s) for s in range(2)]
            for s in range(2):
                start_block(f_base + f + s + N_ROW_SLOTS - 2)
            return slots

        ups = [wait_up(0), wait_up(1)]
        up_part(ups[0])
        gelu_part(0)
        up_part(ups[1])

        def f_body(g, _):
            downs = next_down(2 * g)
            ups = [wait_up(2 * g + 2 + s) for s in range(2)]
            for s in range(2):
                nxt = 2 * g + N_UP_SLOTS + s
                pl.when(nxt < n_f)(functools.partial(start_up, nxt))
            for s in range(2):
                gelu_part(1 - s)
                down_part(downs[s], s)
                up_part(ups[s])
            return 0

        lax.fori_loop(0, n_f // 2 - 1, f_body, 0)
        downs = next_down(n_f - 2)
        gelu_part(1)
        down_part(downs[0], 0)
        down_part(downs[1], 1)
        start_block(q_base + N_ROW_SLOTS - 2)

        def y_body(i, _):
            sl = pl.ds(pl.multiple_of(i * 64, 64), 64)
            y = acc_ref[sl, :].astype(jnp.bfloat16)
            x_ref[sl, :] = y
            if with_qkv:
                yf = y.astype(jnp.float32)
                ms = jnp.mean(yf * yf, axis=-1, keepdims=True)
                n_ref[sl, :] = (yf * lax.rsqrt(ms + NORM_EPS) * ga_ref[layer]).astype(jnp.bfloat16)
            return 0

        lax.fori_loop(0, rows // 64, y_body, 0)
        y_copy = pltpu.make_async_copy(x_ref, y_hbm.at[pl.ds(y_row, rows)], out_sem.at[0])
        y_copy.start()
    else:
        x_copy.wait()
        norm_rows(x_ref, ga_ref[layer], n_ref, rows)

    if with_qkv:
        reps = rows // seq_loc

        def project(b):
            slot = wait_block(b)
            start_block(b + N_ROW_SLOTS - 1)
            return lax.dot_general(n_ref[...], ring[slot], (((1,), (1,)), ((), ())), preferred_element_type=jnp.float32)

        def rope(t, cos_t, sin_t):
            r3 = t.reshape(reps, seq_loc, 128)
            s3 = pltpu.roll(t, 64, 1).reshape(reps, seq_loc, 128)
            return (r3 * cos_t + s3 * sin_t).reshape(rows, 128).astype(jnp.bfloat16)

        def drain(s, dst):
            pltpu.make_async_copy(st_ref.at[s], dst, out_sem.at[1 + s]).wait()

        def q_body(j, _):
            s = lax.rem(j, 2)

            @pl.when(j >= 2)
            def _():
                drain(s, q_hbm.at[:, pl.ds(0, BLK)])

            res = project(q_base + j)
            for i in range(4):
                st_ref[s, :, i * 128 : (i + 1) * 128] = rope(res[:, i * 128 : (i + 1) * 128], tab_ref[0], tab_ref[1])
            pltpu.make_async_copy(
                st_ref.at[s], q_hbm.at[:, pl.ds(pl.multiple_of(j * BLK, BLK), BLK)], out_sem.at[1 + s]
            ).start()
            return 0

        if with_q:
            lax.fori_loop(0, n_q, q_body, 0)
        if with_kv:
            if with_q:
                drain(0, q_hbm.at[:, pl.ds(0, BLK)])
            kres = project(q_base + n_q)
            for i in range(4):
                st_ref[0, :, i * 128 : (i + 1) * 128] = rope(kres[:, i * 128 : (i + 1) * 128], tab_ref[2], tab_ref[3])
            pltpu.make_async_copy(st_ref.at[0], kv_hbm.at[:, pl.ds(0, BLK)], out_sem.at[1]).start()
            if with_q:
                drain(1, q_hbm.at[:, pl.ds(0, BLK)])
            vres = project(q_base + n_q + 1)
            st_ref[1] = vres.astype(jnp.bfloat16)
            pltpu.make_async_copy(st_ref.at[1], kv_hbm.at[:, pl.ds(BLK, BLK)], out_sem.at[2]).start()
            drain(0, kv_hbm.at[:, pl.ds(0, BLK)])
            drain(1, kv_hbm.at[:, pl.ds(BLK, BLK)])
        else:
            drain(0, q_hbm.at[:, pl.ds(0, BLK)])
            drain(1, q_hbm.at[:, pl.ds(0, BLK)])
    if with_mlp:
        y_copy.wait()


def layer_call(
    layer, x, x_row, rows, attn_in, weights, tables, seq_loc, n_dev, with_q, with_kv, y_rows=None, y_row=0, y_into=None
):
    w_query_t, w_key_t, w_value_t, w_out, w_up, w_down, g_attn, g_mlp = weights
    d_model = x.shape[1]
    ff_dim = w_up.shape[2]
    with_mlp = attn_in is not None
    any_spec = pl.BlockSpec(memory_space=pl.ANY)
    vmem_spec = pl.BlockSpec(memory_space=pltpu.VMEM)
    args, specs = [x], [any_spec]
    outs = []
    flops = 0
    nbytes = 0
    if with_mlp:
        q, kv, mask = attn_in
        args += [q, kv, mask, w_out, w_up, w_down, g_mlp]
        specs += [any_spec] * 2 + [vmem_spec] + [any_spec] * 3 + [vmem_spec]
        outs.append(jax.ShapeDtypeStruct((y_rows or rows, d_model), jnp.bfloat16))
        flops += 2 * rows * d_model * (d_model + 2 * ff_dim) + 16 * rows * d_model * n_dev * seq_loc
        nbytes += 2 * d_model * (d_model + 2 * ff_dim) + 6 * rows * d_model + 2 * kv.size
    if with_q or with_kv:
        args += [w_query_t, w_key_t, w_value_t, g_attn, tables]
        specs += [any_spec] * 3 + [vmem_spec] * 2
        n_out = (d_model if with_q else 0) + (2 * BLK if with_kv else 0)
        flops += 2 * rows * d_model * n_out
        nbytes += 2 * d_model * n_out + 2 * rows * n_out
    if with_q:
        outs.append(jax.ShapeDtypeStruct((rows, d_model), jnp.bfloat16))
    if with_kv:
        outs.append(jax.ShapeDtypeStruct((rows, 2 * BLK), jnp.bfloat16))
    aliases = {}
    if y_into is not None:
        aliases = {len(args): 0}
        args.append(y_into)
        specs.append(any_spec)
    scratch = [
        pltpu.VMEM((rows, d_model), jnp.bfloat16),
        pltpu.VMEM((rows, d_model), jnp.bfloat16),
        pltpu.VMEM((N_ROW_SLOTS, BLK, d_model), jnp.bfloat16),
        pltpu.SemaphoreType.DMA((N_ROW_SLOTS,)),
        pltpu.SemaphoreType.DMA,
        pltpu.SemaphoreType.DMA((3,)),
    ]
    if with_mlp:
        scratch += [
            pltpu.VMEM((d_model // BLK, rows, BLK), jnp.bfloat16),
            pltpu.VMEM((rows, d_model), jnp.float32),
            pltpu.VMEM((rows, BLK), jnp.float32),
            pltpu.VMEM((2, rows, BLK), jnp.bfloat16),
            pltpu.VMEM((N_UP_SLOTS, d_model, BLK), jnp.bfloat16),
            pltpu.SemaphoreType.DMA((N_UP_SLOTS,)),
            pltpu.VMEM((rows, d_model), jnp.bfloat16),
            pltpu.SemaphoreType.DMA,
            pltpu.VMEM((N_KV_SLOTS, n_dev, seq_loc, 2 * BLK), jnp.bfloat16),
            pltpu.SemaphoreType.DMA((N_KV_SLOTS,)),
        ]
    if with_q or with_kv:
        scratch.append(pltpu.VMEM((2, rows, BLK), jnp.bfloat16))
    return pl.pallas_call(
        functools.partial(
            layer_kernel, layer, with_mlp, with_q, with_kv, rows, seq_loc, n_dev, d_model, ff_dim, x_row, y_row,
            y_into is not None,
        ),
        out_shape=outs,
        in_specs=specs,
        out_specs=[any_spec] * len(outs),
        scratch_shapes=scratch,
        input_output_aliases=aliases,
        compiler_params=pltpu.CompilerParams(vmem_limit_bytes=60 * 1024 * 1024),
        cost_estimate=pl.CostEstimate(flops=flops, bytes_accessed=nbytes, transcendentals=0),
        name=f"layer_{int(with_mlp)}{int(with_q)}{int(with_kv)}",
    )(*args)


def solution(mesh):
    tok_spec = P(None, ("data", "seq"), None)
    in_specs = (tok_spec, P(("data", "seq"))) + (P(),) * 8

    def device_fn(x_loc, pos_loc, w_query, w_key, w_value, w_out, w_up, w_down, g_attn, g_mlp):
        n_batch, seq_loc, d_model = x_loc.shape
        n_layers = w_query.shape[0]
        n_dev = mesh.shape["seq"]
        scale = w_query.shape[-1] ** -0.5
        cos_t, sin_t = rope_tables(pos_loc, w_query.shape[-1])
        cos4 = jnp.concatenate([cos_t] * 4, axis=-1)
        sin4 = jnp.concatenate([-sin_t, -sin_t, sin_t, sin_t], axis=-1)
        tables = jnp.stack([cos4 * scale, sin4 * scale, cos4, sin4])
        me = lax.axis_index("seq")
        key_pos = jnp.arange(n_dev * seq_loc)
        query_pos = me * seq_loc + jnp.arange(seq_loc)
        mask = jnp.where(key_pos[:, None] <= query_pos[None, :], 0.0, MASK_VALUE)
        mask = jnp.pad(mask, ((0, 0), (0, 128 - seq_loc))).astype(jnp.bfloat16)
        weights = (
            jnp.transpose(w_query, (0, 2, 3, 1)),
            jnp.transpose(w_key, (0, 2, 3, 1)),
            jnp.transpose(w_value, (0, 2, 3, 1)),
            w_out,
            w_up,
            w_down,
            g_attn,
            g_mlp,
        )
        rows = n_batch // N_CHUNKS * seq_loc
        x_all = x_loc.reshape(n_batch * seq_loc, d_model)
        xs = [(x_all, c * rows) for c in range(N_CHUNKS)]
        qs, kvs = [None] * N_CHUNKS, [None] * N_CHUNKS
        call = functools.partial(layer_call, weights=weights, tables=tables, seq_loc=seq_loc, n_dev=n_dev, rows=rows)
        last = None
        for c in range(N_CHUNKS):
            x_c = x_all
            if last is not None:
                x_c, _ = lax.optimization_barrier((x_all, last))
            (kv,) = call(0, x_c, c * rows, attn_in=None, with_q=False, with_kv=True)
            kvs[c] = lax.all_gather(kv, "seq", axis=0, tiled=False)
            last = kv
        for c in range(N_CHUNKS):
            x_c, _ = lax.optimization_barrier((x_all, last))
            (qs[c],) = call(0, x_c, c * rows, attn_in=None, with_q=True, with_kv=False)
            last = qs[c]
        out = None
        for layer in range(1, n_layers + 1):
            for c in range(N_CHUNKS):
                q_c, last = lax.optimization_barrier((qs[c], last))
                attn_in = (q_c, kvs[c], mask)
                if layer < n_layers:
                    y, qs[c], kv = call(layer, *xs[c], attn_in=attn_in, with_q=True, with_kv=True)
                    xs[c] = (y, 0)
                    kvs[c] = lax.all_gather(kv, "seq", axis=0, tiled=False)
                    last = y
                else:
                    (out,) = call(
                        layer, *xs[c], attn_in=attn_in, with_q=False, with_kv=False,
                        y_rows=n_batch * seq_loc, y_row=c * rows, y_into=out,
                    )
                    last = out
        return out.reshape(n_batch, seq_loc, d_model)

    return jax.shard_map(device_fn, mesh=mesh, in_specs=in_specs, out_specs=tok_spec, check_vma=False)
```
